32 devices in a mesh: dp: 4 (over y, x), expert: 4 (over z), tensor: 2 (over core).
Axes of the slice: x: 2, y: 2, z: 4, core: 2. Of those that a mesh axis runs over, the one named last changes fastest.
Arguments:
- tokens: bfloat16 [2048, 2048], P(('dp', 'expert'), 'tensor'), may hold values from -6 to 6
- norm_gain: bfloat16 [2048], replicated, may hold values from 0.25 to 1.75
- expert_ids: int32 [2048, 2], P(('dp', 'expert')), may hold values from 0 to 3, all different within a row; in each aligned block of 128 rows (0 to 127, 128 to 255, ...) at most 128 rows name the same one
- gate_codes: int32 [2048, 2], P(('dp', 'expert')), may hold values from 1 to 255
- gate_weights: bfloat16 [4, 7168, 2048], P('expert', ('dp', 'tensor')), may hold values from -0.125 to 0.125
- up_weights: bfloat16 [4, 7168, 2048], P('expert', ('dp', 'tensor')), may hold values from -0.125 to 0.125
- down_weights: bfloat16 [4, 7168, 2048], P('expert', ('dp', 'tensor')), may hold values from -0.0625 to 0.0625
- value_head: bfloat16 [2048, 128], replicated, may hold values from -0.125 to 0.125
- actions: int32 [2048], P(('dp', 'expert')), may hold values from 0 to 127
- rewards: int32 [2048], P(('dp', 'expert')), may hold values from -8 to 8
- trace_codes: int32 [2048], P(('dp', 'expert')), may hold values from 1 to 1024
Outputs:
- action_values: float32 [2048, 128], P(('dp', 'expert'))
- retrace_targets: float32 [2048], P(('dp', 'expert'))
The draws below stay inside these ranges and needn't reach their ends.
Inputs may be any that keep to these rules, and one draw needn't show every extreme that they name: `expert_ids`: each row names 2 different experts; within the 128 rows of one index pair of dp and expert each expert is named by at most 128 rows, and in some of these blocks one expert by exactly 128.
All inputs are finite; a program needn't handle non-finite values.
Results may differ from the reference program's by a relative error of at most 0.005.
Values may be sent and summed in bfloat16 or wider, within the bound.
A program may use at most 256 MiB of HBM per device.

```python
import math
import jax
import jax.numpy as jnp
import numpy as np
from jax import lax

D = 2048
FF = 7168
TOP = 2
NACT = 128
STEPS = 128
EXPERTS = 4
TOK_GRP = 128
CAP = 128
TOKENS = 2048


def draw_trace_codes(key, part):
    count = TOKENS // STEPS
    key_class = jax.random.fold_in(key, 11)
    key_plain = jax.random.fold_in(key, 12)
    key_where = jax.random.fold_in(key, 13)
    key_depth = jax.random.fold_in(key, 14)
    forgetful = jax.random.randint(key_class, (count, 1), 0, 4) == 0
    plain_codes = jax.random.randint(key_plain, (count, STEPS), 1, 1025)
    lowered = jax.random.randint(key_where, (count, STEPS), 0, 64) == 0
    depth_codes = jax.random.randint(key_depth, (count, STEPS), 768, 1025)
    kept_codes = jnp.where(lowered, depth_codes, 1024)
    codes = jnp.where(forgetful, plain_codes, kept_codes)
    return codes.reshape(-1).astype(jnp.int32)


def set_ends(values, rng, least, top_value):
    spot = [jax.random.randint(jax.random.fold_in(rng, axis), (), 0, length) for axis, length in enumerate(values.shape)]
    longest = values.shape.index(max(values.shape))
    beside = spot[:longest] + [(spot[longest] + 1) % values.shape[longest]] + spot[longest + 1:]
    return values.at[tuple(spot)].set(least).at[tuple(beside)].set(top_value)


def block_levels(key, extent, cuts, least, largest):
    level, own = 1.0, jax.random.fold_in(key, 6)
    for dim, shards_of in cuts:
        heights = jnp.exp(jax.random.uniform(jax.random.fold_in(own, dim), (shards_of,), jnp.float32, least / len(cuts), largest / len(cuts)))
        level = level * jnp.repeat(heights, extent[dim] // shards_of).reshape([-1 if axis == dim else 1 for axis in range(len(extent))])
    return level


def deal_out(stream_key, own, number, rows, count, top, most, skew):
    ranking = jax.random.permutation(stream_key, count)
    heavy_load, usual = portions_of(count, rows * top, most, skew, True), portions_of(count, rows * top, most, skew, False)
    places = jnp.arange(count)

    def named(lengths, turn):
        used = int((lengths > 0).sum())
        fixed = max(1, used // 4)
        passed = fixed + (places - fixed + turn * (used - fixed)) % max(1, count - fixed)
        return jnp.zeros((count,), jnp.int32).at[ranking[jnp.where(places < fixed, places, passed)]].set(jnp.asarray(lengths, jnp.int32))

    lengths = jnp.where(number % 4 == 0, named(heavy_load, number // 4), named(usual, number - number // 4 - 1))
    mixed = jax.random.permutation(jax.random.fold_in(own, 3), count)
    giver, receiver = mixed[0:count // 2 * 2:2], mixed[1:count // 2 * 2:2]
    room = jnp.minimum(lengths[giver] - 1, most - lengths[receiver]) // 2
    room = jnp.where((giver == ranking[0]) | (receiver == ranking[0]) | (lengths[receiver] == 0), 0, jnp.maximum(room, 0))
    passed = jax.random.randint(jax.random.fold_in(own, 4), (count // 2,), 0, 1 << 20) % (room + 1)
    lengths = lengths.at[giver].add(-passed).at[receiver].add(passed)
    items = jnp.searchsorted(jnp.cumsum(lengths), jnp.arange(rows * top), side="right").astype(jnp.int32)
    table = items.reshape(top, rows).T
    table = table[jax.random.permutation(jax.random.fold_in(own, 1), rows)]
    turn = jax.random.randint(jax.random.fold_in(own, 2), (rows, 1), 0, top)
    return jnp.take_along_axis(table, (jnp.arange(top)[None, :] + turn) % top, axis=1)


def portions_of(number_of, total, most, slope, full):
    loads = [(1 << 20) // math.isqrt(standing ** slope) + 1 for standing in range(1, number_of + 1)]
    largest = most if full else min(most, max(-(-total // number_of), total * loads[0] // sum(loads)))
    least = 1 if total - largest >= number_of - 1 else 0
    given, surplus = [largest] + [least] * (number_of - 1), total - largest - least * (number_of - 1)
    while surplus > 0:
        candidates = [i for i in range(1, number_of) if given[i] < largest] or [i for i in range(1, number_of) if given[i] < most]
        whole, remaining = sum([loads[i] for i in candidates]), surplus
        for i in candidates:
            addition = min(most - given[i], max(1, remaining * loads[i] // whole), surplus)
            given[i] = given[i] + addition
            surplus = surplus - addition
    return np.array(given)


def scatter_about(rng, extent, width, bound, shards=(), kind=jnp.bfloat16):
    values = jax.random.normal(rng, extent, jnp.float32) * width
    if len(shards) > 0:
        values = block_levels(rng, extent, shards, -0.22, 0.18) * values
    return jnp.clip(values, min=-bound, max=bound).astype(kind)


def setup_inputs(seed: int = 0) -> dict:
    key_list = jax.random.split(jax.random.key(seed), 12)
    tokens = scatter_about(key_list[0], (TOKENS, D), 1.0, 6.0, ((0, 16), (1, 2)))
    norm_gain = jnp.clip(1.0 + 0.15 * jax.random.normal(key_list[1], (D,), jnp.float32), 0.25, 1.75).astype(jnp.bfloat16)
    expert_ids_keys = jax.random.split(jax.random.fold_in(key_list[2], 1), TOKENS // TOK_GRP)
    expert_ids_turns = jax.random.permutation(jax.random.fold_in(key_list[2], 3), TOKENS // TOK_GRP)
    expert_ids = jax.vmap(lambda own, number: deal_out(jax.random.fold_in(key_list[2], 2), own, number, TOK_GRP, EXPERTS, TOP, CAP, 2))(expert_ids_keys, expert_ids_turns).reshape((TOKENS, TOP))
    gate_codes = set_ends(jax.random.randint(key_list[3], (TOKENS, TOP), 1, 256), jax.random.fold_in(key_list[3], 1), 1, 255).astype(jnp.int32)
    gate_weights = scatter_about(key_list[4], (EXPERTS, FF, D), D ** -0.5, 0.125, ((0, 4), (1, 8)))
    up_weights = scatter_about(key_list[5], (EXPERTS, FF, D), D ** -0.5, 0.125, ((0, 4), (1, 8)))
    down_weights = scatter_about(key_list[6], (EXPERTS, FF, D), FF ** -0.5, 0.0625, ((0, 4), (1, 8)))
    value_head = scatter_about(key_list[7], (D, NACT), D ** -0.5, 0.125)
    actions = set_ends(jax.random.randint(key_list[8], (TOKENS,), 0, NACT), jax.random.fold_in(key_list[8], 1), 0, NACT - 1).astype(jnp.int32)
    rewards = set_ends(jax.random.randint(key_list[9], (TOKENS,), -8, 9), jax.random.fold_in(key_list[9], 1), -8, 8).astype(jnp.int32)
    trace_codes = draw_trace_codes(jax.random.fold_in(key_list[11], 71), 0)
    return dict(tokens=tokens, norm_gain=norm_gain, expert_ids=expert_ids, gate_codes=gate_codes, gate_weights=gate_weights, up_weights=up_weights, down_weights=down_weights, value_head=value_head, actions=actions, rewards=rewards, trace_codes=trace_codes)


DISCOUNT = 0.99
EPSILON = 1e-05

def expert_rows(row_block, gate_matrix, lift_matrix, down_matrix):
    gate_value = lax.dot_general(row_block, gate_matrix, (((1,), (1,)), ((), ())), preferred_element_type=jnp.float32)
    lift_value = lax.dot_general(row_block, lift_matrix, (((1,), (1,)), ((), ())), preferred_element_type=jnp.float32)
    hidden = (jax.nn.silu(gate_value) * lift_value).astype(jnp.bfloat16)
    return jnp.dot(hidden, down_matrix, preferred_element_type=jnp.float32)

def retrace(action_values, actions, rewards, trace_codes):
    greedy = lax.optimization_barrier(jnp.max(action_values, axis=1))
    picked = (actions[:, None] == jnp.arange(action_values.shape[1], dtype=jnp.int32)[None, :]).astype(jnp.float32)
    taken = lax.optimization_barrier(jnp.sum(action_values * picked, axis=1))
    trace = trace_codes.astype(jnp.float32) / 1024.0
    reward = rewards.astype(jnp.float32) * 0.25
    greedy = greedy.reshape(-1, STEPS)
    taken = taken.reshape(-1, STEPS)
    trace = trace.reshape(-1, STEPS)
    reward = reward.reshape(-1, STEPS)
    padding = jnp.zeros_like(greedy[:, :1])
    greedy_next = jnp.concatenate([greedy[:, 1:], padding], axis=1)
    taken_next = jnp.concatenate([taken[:, 1:], padding], axis=1)
    trace_next = jnp.concatenate([trace[:, 1:], padding], axis=1)
    driver = reward + DISCOUNT * (greedy_next - trace_next * taken_next)
    log_sums = jnp.cumsum(jnp.log(DISCOUNT * trace), axis=1)
    spans = log_sums[:, None, :] - log_sums[:, :, None]
    upper_mask = jnp.arange(STEPS, dtype=jnp.int32)[None, :] >= jnp.arange(STEPS, dtype=jnp.int32)[:, None]
    weight = jnp.where(upper_mask[None, :, :], jnp.exp(jnp.minimum(spans, 0.0)), 0.0)
    target = jnp.einsum('nts,ns->nt', weight, driver, precision=lax.Precision.HIGHEST)
    return target.reshape(-1)

def reference(tokens, norm_gain, expert_ids, gate_codes, gate_weights, up_weights, down_weights, value_head, actions, rewards, trace_codes):
    widened = tokens.astype(jnp.float32)
    scaling = lax.rsqrt(lax.optimization_barrier(jnp.mean(widened * widened, axis=1, keepdims=True)) + EPSILON)
    normed = (widened * scaling * norm_gain.astype(jnp.float32)[None, :]).astype(jnp.bfloat16)
    codes = gate_codes.astype(jnp.float32)
    gate_share = codes / lax.optimization_barrier(jnp.sum(codes, axis=1, keepdims=True))
    row_limit = TOKENS // TOK_GRP * CAP

    def one_expert(running, inputs):
        expert_index, gate_matrix, lift_matrix, down_matrix = inputs
        matched = expert_ids == expert_index
        share = lax.optimization_barrier(jnp.sum(jnp.where(matched, gate_share, 0.0), axis=1))
        chosen = jnp.any(matched, axis=1)
        chosen_rows = jnp.nonzero(chosen, size=row_limit, fill_value=0)[0].astype(jnp.int32)
        amount = jnp.sum(chosen.astype(jnp.int32))
        in_range = (jnp.arange(row_limit, dtype=jnp.int32) < amount).astype(jnp.float32)
        output = expert_rows(normed[chosen_rows], gate_matrix, lift_matrix, down_matrix)
        running = running.at[chosen_rows].add(output * (share[chosen_rows] * in_range)[:, None])
        return (running, None)
    start_sum = jnp.zeros((TOKENS, D), jnp.float32)
    blended, _ = lax.scan(one_expert, start_sum, (jnp.arange(EXPERTS, dtype=jnp.int32), gate_weights, up_weights, down_weights))
    action_values = jnp.dot(blended, value_head.astype(jnp.float32), precision=lax.Precision.HIGHEST, preferred_element_type=jnp.float32)
    retrace_targets = retrace(action_values, actions, rewards, trace_codes)
    return (action_values, retrace_targets)
```

```python
import jax
import jax.numpy as jnp
from jax import lax
from jax.experimental import pallas as pl
from jax.experimental.pallas import tpu as pltpu
from jax.sharding import PartitionSpec as P

TOP = 2
STEPS = 128


DISCOUNT = 0.99
EPSILON = 1e-05


def expert_rows(row_block, gate_matrix, lift_matrix, down_matrix):
    gate_value = lax.dot_general(
        row_block, gate_matrix, (((1,), (1,)), ((), ())), preferred_element_type=jnp.float32
    )
    lift_value = lax.dot_general(
        row_block, lift_matrix, (((1,), (1,)), ((), ())), preferred_element_type=jnp.float32
    )
    hidden = (jax.nn.silu(gate_value) * lift_value).astype(jnp.bfloat16)
    return jnp.dot(hidden, down_matrix, preferred_element_type=jnp.float32)


def retrace(action_values, actions, rewards, trace_codes):
    greedy = jnp.max(action_values, axis=1)
    picked = (
        actions[:, None] == jnp.arange(action_values.shape[1], dtype=jnp.int32)[None, :]
    ).astype(jnp.float32)
    taken = jnp.sum(action_values * picked, axis=1)
    trace = trace_codes.astype(jnp.float32) / 1024.0
    reward = rewards.astype(jnp.float32) * 0.25
    greedy = greedy.reshape(-1, STEPS)
    taken = taken.reshape(-1, STEPS)
    trace = trace.reshape(-1, STEPS)
    reward = reward.reshape(-1, STEPS)
    padding = jnp.zeros_like(greedy[:, :1])
    greedy_next = jnp.concatenate([greedy[:, 1:], padding], axis=1)
    taken_next = jnp.concatenate([taken[:, 1:], padding], axis=1)
    trace_next = jnp.concatenate([trace[:, 1:], padding], axis=1)
    driver = reward + DISCOUNT * (greedy_next - trace_next * taken_next)
    log_sums = jnp.cumsum(jnp.log(DISCOUNT * trace), axis=1)
    spans = log_sums[:, None, :] - log_sums[:, :, None]
    upper_mask = (
        jnp.arange(STEPS, dtype=jnp.int32)[None, :] >= jnp.arange(STEPS, dtype=jnp.int32)[:, None]
    )
    weight = jnp.where(upper_mask[None, :, :], jnp.exp(jnp.minimum(spans, 0.0)), 0.0)
    target = jnp.einsum("nts,ns->nt", weight, driver, precision=lax.Precision.HIGHEST)
    return target.reshape(-1)


def per_device_plain(
    tokens,
    norm_gain,
    expert_ids,
    gate_codes,
    gate_weights,
    up_weights,
    down_weights,
    value_head,
    actions,
    rewards,
    trace_codes,
):
    mesh_rows = ("dp", "expert")
    expert = lax.axis_index("expert")
    codes = gate_codes.astype(jnp.float32)
    gate_share = codes / jnp.sum(codes, axis=1, keepdims=True)
    experts = jnp.arange(lax.axis_size("expert"), dtype=jnp.int32)
    share = jnp.sum(
        jnp.where(expert_ids[:, :, None] == experts[None, None, :], gate_share[:, :, None], 0.0),
        axis=1,
    )
    every_share = lax.all_gather(share, mesh_rows, axis=0, tiled=True)
    own_share = lax.dynamic_slice_in_dim(every_share, expert, 1, axis=1)
    full = lax.all_gather(tokens, "tensor", axis=1, tiled=True)
    widened = full.astype(jnp.float32)
    scaling = lax.rsqrt(jnp.mean(widened * widened, axis=1, keepdims=True) + EPSILON)
    normed = (widened * scaling * norm_gain.astype(jnp.float32)[None, :]).astype(jnp.bfloat16)
    gathered = lax.all_gather(normed, mesh_rows, axis=0, tiled=True)
    scored = jnp.dot(down_weights[0], value_head, preferred_element_type=jnp.float32)
    high = scored.astype(jnp.bfloat16)
    low = (scored - high.astype(jnp.float32)).astype(jnp.bfloat16)
    both = jnp.concatenate([high, low], axis=1)
    wide = expert_rows(gathered, gate_weights[0], up_weights[0], both)
    actions_count = value_head.shape[1]
    partial_values = (wide[:, :actions_count] + wide[:, actions_count:]) * own_share
    partial_values = lax.psum_scatter(partial_values, mesh_rows, scatter_dimension=0, tiled=True)
    action_values = lax.psum(partial_values, "tensor")
    retrace_targets = retrace(action_values, actions, rewards, trace_codes)
    return (action_values, retrace_targets)


RING = 4
MESH = pl.DeviceIdType.MESH
TILE = 128
FIRST = ((0, 0), (1, 0), (3, 0), (0, 1), (0, 3))
SECOND = ((1, 1), (1, 3), (3, 1), (3, 3))
THIRD = ((2, 0), (0, 2), (2, 1), (1, 2))
FOURTH = ((2, 3), (3, 2), (2, 2))
GROUPS = (FIRST, SECOND, THIRD, FOURTH)


def gray(place):
    return place + (place // 2) * (1 - 2 * (place % 2))


def critic_kernel(
    tokens_ref,
    gain_ref,
    ids_ref,
    codes_ref,
    gate_ref,
    up_ref,
    down_ref,
    head_ref,
    actions_ref,
    rewards_ref,
    trace_ref,
    values_ref,
    targets_ref,
    raw,
    near,
    far,
    gate_buf,
    up_buf,
    down_buf,
    scored_buf,
    hidden_buf,
    sent,
    landed,
    share_buf,
    halves,
    load_sems,
    pair_send,
    pair_recv,
    ring_send,
    ring_recv,
    swap_send,
    swap_recv,
    back_send,
    back_recv,
):
    dp = lax.axis_index("dp")
    z = lax.axis_index("expert")
    core = lax.axis_index("tensor")
    other = 1 - core
    p = gray(dp)
    rows = tokens_ref.shape[0]
    half_rows = rows // 2
    part = near.shape[-1]
    wide = tokens_ref.shape[1]
    hidden_units = gate_ref.shape[1]
    actions_count = head_ref.shape[1]

    def device(step_p, step_z, which):
        return (gray((p + step_p) % RING), (z + step_z) % RING, which)

    load_token = pltpu.make_async_copy(tokens_ref, raw.at[core], load_sems.at[0])
    load_down = pltpu.make_async_copy(down_ref.at[0], down_buf, load_sems.at[1])
    load_gate = pltpu.make_async_copy(gate_ref.at[0], gate_buf, load_sems.at[2])
    load_up = pltpu.make_async_copy(up_ref.at[0], up_buf, load_sems.at[3])
    load_token.start()
    load_down.start()
    load_gate.start()
    load_up.start()

    barrier = pltpu.get_barrier_semaphore()
    for step_p in range(RING):
        for step_z in range(RING):
            for which in range(2):
                if (step_p, step_z, which) != (0, 0, 0):
                    pl.semaphore_signal(
                        barrier,
                        inc=1,
                        device_id=device(step_p, step_z, (core + which) % 2),
                        device_id_type=MESH,
                    )
    pl.semaphore_wait(barrier, 2 * RING * RING - 1)

    sends = []

    def send(source, target, send_sem, recv_sem, to):
        copy = pltpu.make_async_remote_copy(
            src_ref=source,
            dst_ref=target,
            send_sem=send_sem,
            recv_sem=recv_sem,
            device_id=to,
            device_id_type=MESH,
        )
        copy.start()
        sends.append(copy)

    def await_in(target, recv_sem):
        pltpu.make_async_remote_copy(
            src_ref=target,
            dst_ref=target,
            send_sem=recv_sem,
            recv_sem=recv_sem,
            device_id=device(0, 0, other),
            device_id_type=MESH,
        ).wait_recv()

    load_token.wait()
    send(raw.at[core], raw.at[core], pair_send.at[0], pair_recv.at[0], device(0, 0, other))
    first_axis = lax.broadcasted_iota(jnp.int32, (rows, rows), 0)
    second_axis = lax.broadcasted_iota(jnp.int32, (rows, rows), 1)
    same = first_axis == second_axis

    def column(row):
        return jnp.sum(jnp.where(same, row, 0.0), axis=1, keepdims=True)

    def row_of(col):
        return jnp.sum(jnp.where(same, col, 0.0), axis=0, keepdims=True)

    codes = codes_ref[...].astype(jnp.float32)
    gate_share = codes / jnp.sum(codes, axis=0, keepdims=True)
    ids = ids_ref[...]
    for expert in range(RING):
        share = jnp.sum(jnp.where(ids == expert, gate_share, 0.0), axis=0, keepdims=True)
        share_buf[expert] = jnp.broadcast_to(column(share), (rows, actions_count))

    await_in(raw.at[other], pair_recv.at[0])
    left = raw[0].astype(jnp.float32)
    right = raw[1].astype(jnp.float32)
    total = jnp.sum(left * left, axis=1, keepdims=True) + jnp.sum(
        right * right, axis=1, keepdims=True
    )
    scaling = lax.rsqrt(total / (2 * wide) + EPSILON)
    gain = gain_ref[...].astype(jnp.float32)
    for number, widened in enumerate((left, right)):
        normed = (widened * scaling * gain[:, number * wide : (number + 1) * wide]).astype(
            jnp.bfloat16
        )
        near[number, z, p] = normed[:, :part]
        far[number, p, z] = normed[:, part:]

    def block(kind, which, step_f, step_g):
        if kind == 0:
            return near.at[which, (z + step_g) % RING, (p + step_f) % RING]
        return far.at[which, (p + step_g) % RING, (z + step_f) % RING]

    def peer(kind, step_f, step_g):
        if kind == 0:
            return device(step_f, step_g, core)
        return device(step_g, step_f, core)

    def number_of(step_f, step_g):
        return step_g * RING + step_f

    half = (pl.ds(0, half_rows), pl.ds(half_rows, half_rows))

    def relay(kind, step_f, step_g, by_f, by_g, slot=None, cut=None):
        source = block(kind, core, step_f, step_g)
        seen = number_of((step_f - by_f) % RING, (step_g - by_g) % RING)
        if cut is not None:
            source = source.at[half[cut]]
            seen = RING * RING if cut == 1 else seen
        send(
            source,
            source,
            ring_send.at[kind, seen],
            ring_recv.at[kind, seen],
            peer(kind, by_f, by_g),
        )

    def arrive(kind, step_f, step_g):
        here = block(kind, core, step_f, step_g)
        seen = number_of(step_f, step_g)
        if (step_f, step_g) == (2, 0):
            await_in(here.at[half[0]], ring_recv.at[kind, seen])
            await_in(here.at[half[1]], ring_recv.at[kind, RING * RING])
        else:
            await_in(here, ring_recv.at[kind, seen])

    def swap(kind, step_f, step_g):
        here = block(kind, core, step_f, step_g)
        seen = number_of(step_f, step_g)
        send(
            here,
            here,
            swap_send.at[kind, seen],
            swap_recv.at[kind, seen],
            device(0, 0, other),
        )

    def swapped(kind, step_f, step_g):
        await_in(
            block(kind, other, step_f, step_g), swap_recv.at[kind, number_of(step_f, step_g)]
        )

    for kind in range(2):
        relay(kind, 0, 0, 1, 0)
        relay(kind, 0, 0, 3, 0)
    for kind in range(2):
        relay(kind, 0, 0, 0, 1)
        relay(kind, 0, 0, 0, 3)

    load_down.wait()
    scored = jnp.dot(down_buf[...], head_ref[...], preferred_element_type=jnp.float32)
    high = scored.astype(jnp.bfloat16)
    scored_buf[:, :actions_count] = high
    scored_buf[:, actions_count:] = (scored - high.astype(jnp.float32)).astype(jnp.bfloat16)

    for kind in range(2):
        for step_f in (1, 3):
            arrive(kind, step_f, 0)
            relay(kind, step_f, 0, (4 - step_f) % RING, 0, cut=0 if step_f == 3 else 1)
    for kind in range(2):
        for step_f in (1, 3):
            relay(kind, step_f, 0, 0, 1)
            relay(kind, step_f, 0, 0, 3)
            swap(kind, step_f, 0)
    for kind in range(2):
        arrive(kind, 2, 0)
        relay(kind, 2, 0, 0, 1)
        relay(kind, 2, 0, 0, 3)
        swap(kind, 2, 0)

    rising = (0, 1)

    def take(kind, step_f):
        for step_g in (1, 3):
            arrive(kind, step_f, step_g)
            if (step_g == 3) == (step_f in rising):
                relay(kind, step_f, step_g, 0, (4 - step_g) % RING)
            swap(kind, step_f, step_g)

    def kinds(step_p, step_z):
        return ((0, step_p, step_z), (1, step_z, step_p))

    def compute(group, base):
        for step_p, step_z in group:
            if (step_p, step_z) != (0, 0):
                for kind, step_f, step_g in kinds(step_p, step_z):
                    swapped(kind, step_f, step_g)
        lhs_rows = len(group) * rows

        def tile(index, carry):
            at = pl.ds(pl.multiple_of(index * TILE, TILE), TILE)
            weights = jnp.concatenate([gate_buf[at, :], up_buf[at, :]], axis=0)
            block_rows = []
            for step_p, step_z in group:
                zz, pp = (z + step_z) % RING, (p + step_p) % RING
                block_rows.append(
                    jnp.concatenate(
                        [near[0, zz, pp], far[0, pp, zz], near[1, zz, pp], far[1, pp, zz]],
                        axis=1,
                    )
                )
            lhs = jnp.concatenate(block_rows, axis=0)
            both = lax.dot_general(
                lhs, weights, (((1,), (1,)), ((), ())), preferred_element_type=jnp.float32
            )
            hidden = (jax.nn.silu(both[:, :TILE]) * both[:, TILE:]).astype(jnp.bfloat16)
            hidden_buf[:lhs_rows, at] = hidden
            return carry

        lax.fori_loop(0, hidden_units // TILE, tile, 0)
        result = jnp.dot(
            hidden_buf[:lhs_rows, :], scored_buf[...], preferred_element_type=jnp.float32
        )
        result = (result[:, :actions_count] + result[:, actions_count:]).astype(jnp.bfloat16)
        for place, (step_p, step_z) in enumerate(group):
            slot = base + place
            sent[slot] = result[place * rows : (place + 1) * rows]
            source = number_of((-step_p) % RING, (-step_z) % RING)
            own = (step_p, step_z) == (0, 0)
            if own:
                landed[z, p, core] = sent[
                    slot, pl.ds(pl.multiple_of(core * half_rows, half_rows), half_rows), :
                ]
                targets = ((other, 1),)
            else:
                targets = ((0, core % 2), (1, (core + 1) % 2))
            for which, relative in targets:
                cut = pl.ds(pl.multiple_of(which * half_rows, half_rows), half_rows)
                send(
                    sent.at[slot, cut],
                    landed.at[z, p, core],
                    back_send.at[2 * slot + which],
                    back_recv.at[2 * source + relative],
                    device(step_p, step_z, which),
                )

    for kind in range(2):
        take(kind, 0)
    load_gate.wait()
    load_up.wait()
    compute(FIRST, 0)
    for kind in range(2):
        take(kind, 1)
        take(kind, 3)
    for kind in range(2):
        take(kind, 2)
    compute(SECOND, 5)
    for step_f in range(RING):
        for kind in range(2):
            arrive(kind, step_f, 2)
            swap(kind, step_f, 2)
    compute(THIRD, 9)
    compute(FOURTH, 13)

    for step_p in range(RING):
        for step_z in range(RING):
            for relative in range(2):
                if (step_p, step_z, relative) != (0, 0, 0):
                    await_in(
                        landed.at[
                            (z + step_z) % RING, (p + step_p) % RING, (core + relative) % 2
                        ],
                        back_recv.at[2 * number_of(step_p, step_z) + relative],
                    )
    mine = pl.ds(pl.multiple_of(core * half_rows, half_rows), half_rows)
    blended = jnp.zeros((half_rows, actions_count), jnp.float32)
    for expert in range(RING):
        part_sum = jnp.zeros((half_rows, actions_count), jnp.float32)
        for place in range(RING):
            for which in range(2):
                part_sum = part_sum + landed[expert, place, which].astype(jnp.float32)
        blended = blended + share_buf[expert, mine, :] * part_sum
    halves[core] = blended
    send(
        halves.at[core], halves.at[core], pair_send.at[1], pair_recv.at[1], device(0, 0, other)
    )

    trace_row = trace_ref[...].astype(jnp.float32) / 1024.0
    trace_col = column(trace_row)
    reward_col = column(rewards_ref[...].astype(jnp.float32) * 0.25)
    action_col = column(actions_ref[...].astype(jnp.float32))
    log_row = jnp.log(DISCOUNT * trace_row)
    log_col = column(log_row)
    sums_row = jnp.sum(jnp.where(first_axis <= second_axis, log_col, 0.0), axis=0, keepdims=True)
    sums_col = jnp.sum(jnp.where(second_axis <= first_axis, log_row, 0.0), axis=1, keepdims=True)
    weight = jnp.where(
        first_axis >= second_axis, jnp.exp(jnp.minimum(sums_col - sums_row, 0.0)), 0.0
    )
    action_axis = lax.broadcasted_iota(jnp.int32, (rows, actions_count), 1).astype(jnp.float32)
    chosen = action_axis == action_col

    await_in(halves.at[other], pair_recv.at[1])
    values = jnp.concatenate([halves[0], halves[1]], axis=0)
    values_ref[...] = values
    greedy = jnp.max(values, axis=1, keepdims=True)
    taken = jnp.sum(jnp.where(chosen, values, 0.0), axis=1, keepdims=True)
    ahead_row = row_of(greedy - trace_col * taken)
    ahead = jnp.sum(
        jnp.where(second_axis == first_axis + 1, ahead_row, 0.0), axis=1, keepdims=True
    )
    driver = reward_col + DISCOUNT * ahead
    targets_ref[...] = jnp.sum(weight * driver, axis=0, keepdims=True)
    for copy in sends:
        copy.wait_send()


def per_device(
    tokens,
    norm_gain,
    expert_ids,
    gate_codes,
    gate_weights,
    up_weights,
    down_weights,
    value_head,
    actions,
    rewards,
    trace_codes,
):
    rows, wide = tokens.shape
    hidden_units, features = gate_weights.shape[1:]
    actions_count = value_head.shape[1]
    part = wide // 2
    held = (2, RING, RING, rows, part)
    most = max(len(group) for group in GROUPS) * rows
    vmem = pl.BlockSpec(memory_space=pltpu.VMEM)
    hbm = pl.BlockSpec(memory_space=pltpu.HBM)
    dma = pltpu.SemaphoreType.DMA
    blocks = RING * RING
    values, targets = pl.pallas_call(
        critic_kernel,
        out_shape=(
            jax.ShapeDtypeStruct((rows, actions_count), jnp.float32),
            jax.ShapeDtypeStruct((1, rows), jnp.float32),
        ),
        in_specs=[hbm, vmem, vmem, vmem, hbm, hbm, hbm, vmem, vmem, vmem, vmem],
        out_specs=(vmem, vmem),
        scratch_shapes=[
            pltpu.VMEM((2, rows, wide), jnp.bfloat16),
            pltpu.VMEM(held, jnp.bfloat16),
            pltpu.VMEM(held, jnp.bfloat16),
            pltpu.VMEM((hidden_units, features), jnp.bfloat16),
            pltpu.VMEM((hidden_units, features), jnp.bfloat16),
            pltpu.VMEM((hidden_units, features), jnp.bfloat16),
            pltpu.VMEM((hidden_units, 2 * actions_count), jnp.bfloat16),
            pltpu.VMEM((most, hidden_units), jnp.bfloat16),
            pltpu.VMEM((blocks, rows, actions_count), jnp.bfloat16),
            pltpu.VMEM((RING, RING, 2, rows // 2, actions_count), jnp.bfloat16),
            pltpu.VMEM((RING, rows, actions_count), jnp.float32),
            pltpu.VMEM((2, rows // 2, actions_count), jnp.float32),
            dma((4,)),
            dma((2,)),
            dma((2,)),
            dma((2, blocks + 1)),
            dma((2, blocks + 1)),
            dma((2, blocks)),
            dma((2, blocks)),
            dma((2 * blocks,)),
            dma((2 * blocks,)),
        ],
        compiler_params=pltpu.CompilerParams(
            collective_id=0, has_side_effects=True, vmem_limit_bytes=60 * 1024 * 1024
        ),
    )(
        tokens,
        norm_gain.reshape(1, -1),
        expert_ids.T,
        gate_codes.T,
        gate_weights,
        up_weights,
        down_weights,
        value_head,
        actions.reshape(1, -1),
        rewards.reshape(1, -1),
        trace_codes.reshape(1, -1),
    )
    return values, targets.reshape(-1)


def solution(mesh):
    in_specs = (
        P(("dp", "expert"), "tensor"),
        P(),
        P(("dp", "expert"), None),
        P(("dp", "expert"), None),
        P("expert", ("dp", "tensor"), None),
        P("expert", ("dp", "tensor"), None),
        P("expert", ("dp", "tensor"), None),
        P(),
        P(("dp", "expert")),
        P(("dp", "expert")),
        P(("dp", "expert")),
    )
    out_specs = (P(("dp", "expert"), None), P(("dp", "expert")))
    shape = mesh.shape
    rings = shape["dp"] == RING and shape["expert"] == RING and shape["tensor"] == 2
    body = per_device if rings else per_device_plain
    return jax.shard_map(
        body, mesh=mesh, in_specs=in_specs, out_specs=out_specs, check_vma=False
    )
```

```python
import jax
import jax.numpy as jnp
from jax import lax
from jax.experimental import pallas as pl
from jax.experimental.pallas import tpu as pltpu
from jax.sharding import PartitionSpec as P

TOP = 2
STEPS = 128


DISCOUNT = 0.99
EPSILON = 1e-05


def expert_rows(row_block, gate_matrix, lift_matrix, down_matrix):
    gate_value = lax.dot_general(
        row_block, gate_matrix, (((1,), (1,)), ((), ())), preferred_element_type=jnp.float32
    )
    lift_value = lax.dot_general(
        row_block, lift_matrix, (((1,), (1,)), ((), ())), preferred_element_type=jnp.float32
    )
    hidden = (jax.nn.silu(gate_value) * lift_value).astype(jnp.bfloat16)
    return jnp.dot(hidden, down_matrix, preferred_element_type=jnp.float32)


def retrace(action_values, actions, rewards, trace_codes):
    greedy = jnp.max(action_values, axis=1)
    picked = (
        actions[:, None] == jnp.arange(action_values.shape[1], dtype=jnp.int32)[None, :]
    ).astype(jnp.float32)
    taken = jnp.sum(action_values * picked, axis=1)
    trace = trace_codes.astype(jnp.float32) / 1024.0
    reward = rewards.astype(jnp.float32) * 0.25
    greedy = greedy.reshape(-1, STEPS)
    taken = taken.reshape(-1, STEPS)
    trace = trace.reshape(-1, STEPS)
    reward = reward.reshape(-1, STEPS)
    padding = jnp.zeros_like(greedy[:, :1])
    greedy_next = jnp.concatenate([greedy[:, 1:], padding], axis=1)
    taken_next = jnp.concatenate([taken[:, 1:], padding], axis=1)
    trace_next = jnp.concatenate([trace[:, 1:], padding], axis=1)
    driver = reward + DISCOUNT * (greedy_next - trace_next * taken_next)
    log_sums = jnp.cumsum(jnp.log(DISCOUNT * trace), axis=1)
    spans = log_sums[:, None, :] - log_sums[:, :, None]
    upper_mask = (
        jnp.arange(STEPS, dtype=jnp.int32)[None, :] >= jnp.arange(STEPS, dtype=jnp.int32)[:, None]
    )
    weight = jnp.where(upper_mask[None, :, :], jnp.exp(jnp.minimum(spans, 0.0)), 0.0)
    target = jnp.einsum("nts,ns->nt", weight, driver, precision=lax.Precision.HIGHEST)
    return target.reshape(-1)


def per_device_plain(
    tokens,
    norm_gain,
    expert_ids,
    gate_codes,
    gate_weights,
    up_weights,
    down_weights,
    value_head,
    actions,
    rewards,
    trace_codes,
):
    mesh_rows = ("dp", "expert")
    expert = lax.axis_index("expert")
    codes = gate_codes.astype(jnp.float32)
    gate_share = codes / jnp.sum(codes, axis=1, keepdims=True)
    experts = jnp.arange(lax.axis_size("expert"), dtype=jnp.int32)
    share = jnp.sum(
        jnp.where(expert_ids[:, :, None] == experts[None, None, :], gate_share[:, :, None], 0.0),
        axis=1,
    )
    every_share = lax.all_gather(share, mesh_rows, axis=0, tiled=True)
    own_share = lax.dynamic_slice_in_dim(every_share, expert, 1, axis=1)
    full = lax.all_gather(tokens, "tensor", axis=1, tiled=True)
    widened = full.astype(jnp.float32)
    scaling = lax.rsqrt(jnp.mean(widened * widened, axis=1, keepdims=True) + EPSILON)
    normed = (widened * scaling * norm_gain.astype(jnp.float32)[None, :]).astype(jnp.bfloat16)
    gathered = lax.all_gather(normed, mesh_rows, axis=0, tiled=True)
    scored = jnp.dot(down_weights[0], value_head, preferred_element_type=jnp.float32)
    high = scored.astype(jnp.bfloat16)
    low = (scored - high.astype(jnp.float32)).astype(jnp.bfloat16)
    both = jnp.concatenate([high, low], axis=1)
    wide = expert_rows(gathered, gate_weights[0], up_weights[0], both)
    actions_count = value_head.shape[1]
    partial_values = (wide[:, :actions_count] + wide[:, actions_count:]) * own_share
    partial_values = lax.psum_scatter(partial_values, mesh_rows, scatter_dimension=0, tiled=True)
    action_values = lax.psum(partial_values, "tensor")
    retrace_targets = retrace(action_values, actions, rewards, trace_codes)
    return (action_values, retrace_targets)


RING = 4
MESH = pl.DeviceIdType.MESH
TILE = 128
ORDER = (0, 1, 3, 2)


def gray(place):
    return place + (place // 2) * (1 - 2 * (place % 2))


def critic_kernel(
    tokens_ref,
    gain_ref,
    ids_ref,
    codes_ref,
    gate_ref,
    up_ref,
    down_ref,
    head_ref,
    actions_ref,
    rewards_ref,
    trace_ref,
    values_ref,
    targets_ref,
    raw,
    near,
    far,
    gate_buf,
    up_buf,
    down_buf,
    scored_buf,
    hidden_buf,
    partial,
    given,
    sent,
    landed,
    share_buf,
    halves,
    load_sems,
    pair_send,
    pair_recv,
    ring_send,
    ring_recv,
    line_send,
    swap_send,
    swap_recv,
    give_send,
    give_recv,
    back_send,
    back_recv,
):
    dp = lax.axis_index("dp")
    z = lax.axis_index("expert")
    core = lax.axis_index("tensor")
    other = 1 - core
    p = gray(dp)
    rows = tokens_ref.shape[0]
    half_rows = rows // 2
    part = near.shape[-1]
    planes = (z, z + 1 - 2 * (z % 2), jnp.where(z < 2, 2, 1), jnp.where(z < 2, 3, 0))
    wide = tokens_ref.shape[1]
    hidden_units = gate_ref.shape[1]
    actions_count = head_ref.shape[1]

    def device(step_p, step_z, which):
        return (gray((p + step_p) % RING), (z + step_z) % RING, which)

    load_token = pltpu.make_async_copy(tokens_ref, raw.at[core], load_sems.at[0])
    load_down = pltpu.make_async_copy(down_ref.at[0], down_buf, load_sems.at[1])
    load_gate = pltpu.make_async_copy(gate_ref.at[0], gate_buf, load_sems.at[2])
    load_up = pltpu.make_async_copy(up_ref.at[0], up_buf, load_sems.at[3])
    load_token.start()
    load_down.start()
    load_gate.start()
    load_up.start()

    barrier = pltpu.get_barrier_semaphore()
    for step_p in range(RING):
        for step_z in range(RING):
            if (step_p, step_z) != (0, 0):
                pl.semaphore_signal(
                    barrier, inc=1, device_id=device(step_p, step_z, core), device_id_type=MESH
                )
    pl.semaphore_signal(barrier, inc=1, device_id=device(0, 0, other), device_id_type=MESH)
    pl.semaphore_wait(barrier, RING * RING)

    sends = []

    def send(source, target, send_sem, recv_sem, to, condition=None):
        def make():
            return pltpu.make_async_remote_copy(
                src_ref=source,
                dst_ref=target,
                send_sem=send_sem,
                recv_sem=recv_sem,
                device_id=to,
                device_id_type=MESH,
            )

        if condition is None:
            make().start()
        else:
            pl.when(condition)(lambda: make().start())
        sends.append((condition, make))

    def await_in(target, recv_sem):
        pltpu.make_async_remote_copy(
            src_ref=target,
            dst_ref=target,
            send_sem=recv_sem,
            recv_sem=recv_sem,
            device_id=device(0, 0, other),
            device_id_type=MESH,
        ).wait_recv()

    load_token.wait()
    send(raw.at[core], raw.at[core], pair_send.at[0], pair_recv.at[0], device(0, 0, other))
    first_axis = lax.broadcasted_iota(jnp.int32, (rows, rows), 0)
    second_axis = lax.broadcasted_iota(jnp.int32, (rows, rows), 1)
    same = first_axis == second_axis

    def column(row):
        return jnp.sum(jnp.where(same, row, 0.0), axis=1, keepdims=True)

    def row_of(col):
        return jnp.sum(jnp.where(same, col, 0.0), axis=0, keepdims=True)

    codes = codes_ref[...].astype(jnp.float32)
    gate_share = codes / jnp.sum(codes, axis=0, keepdims=True)
    ids = ids_ref[...]
    for expert in range(RING):
        share = jnp.sum(jnp.where(ids == expert, gate_share, 0.0), axis=0, keepdims=True)
        share_buf[expert] = jnp.broadcast_to(column(share), (rows, actions_count))

    await_in(raw.at[other], pair_recv.at[0])
    left = raw[0].astype(jnp.float32)
    right = raw[1].astype(jnp.float32)
    total = jnp.sum(left * left, axis=1, keepdims=True) + jnp.sum(
        right * right, axis=1, keepdims=True
    )
    scaling = lax.rsqrt(total / (2 * wide) + EPSILON)
    gain = gain_ref[...].astype(jnp.float32)
    for number, widened in enumerate((left, right)):
        normed = (widened * scaling * gain[:, number * wide : (number + 1) * wide]).astype(
            jnp.bfloat16
        )
        near[number, z, p] = normed[:, :part]
        far[number, z, p] = normed[:, part:]

    buffers = (near, far)
    half = (pl.ds(0, half_rows), pl.ds(half_rows, half_rows))
    lower, upper = z > 0, z < RING - 1
    inner = jnp.logical_and(lower, upper)

    def block(kind, which, plane, step_f):
        return buffers[kind].at[which, plane, (p + step_f) % RING]

    def around(kind, plane, step_f, by, cut=None):
        source = block(kind, core, plane, step_f)
        seen = plane * 5 + (step_f - by) % RING
        if cut is not None:
            source = source.at[half[cut]]
            seen = plane * 5 + (4 if cut == 1 else 2)
        send(
            source,
            source,
            ring_send.at[kind, seen],
            ring_recv.at[kind, seen],
            device(by, 0, core),
        )

    def along(kind, plane, step_f, to, condition, lane):
        source = block(kind, core, plane, step_f)
        send(
            source,
            source,
            line_send.at[kind, lane, plane * RING + step_f],
            ring_recv.at[kind, plane * 5 + step_f],
            (dp, to, core),
            condition,
        )

    def both_ways(kind, step_f):
        along(kind, z, step_f, z + 1, upper, 0)
        along(kind, z, step_f, z - 1, lower, 1)

    def onward(kind, plane, step_f):
        along(kind, plane, step_f, jnp.where(plane < z, z + 1, z - 1), inner, 0)

    def arrive(kind, plane, step_f, split=False):
        here = block(kind, core, plane, step_f)
        if split:
            await_in(here.at[half[0]], ring_recv.at[kind, plane * 5 + 2])
            await_in(here.at[half[1]], ring_recv.at[kind, plane * 5 + 4])
        else:
            await_in(here, ring_recv.at[kind, plane * 5 + step_f])

    def swap(kind, plane, step_f):
        here = block(kind, core, plane, step_f)
        seen = plane * RING + step_f
        send(
            here,
            here,
            swap_send.at[kind, seen],
            swap_recv.at[kind, seen],
            device(0, 0, other),
        )

    def swapped(kind, plane, step_f):
        await_in(block(kind, other, plane, step_f), swap_recv.at[kind, plane * RING + step_f])

    def turn(kind, plane):
        for step_f in (1, 3):
            arrive(kind, plane, step_f)
            around(kind, plane, step_f, (4 - step_f) % RING, cut=0 if step_f == 3 else 1)
        for step_f in (1, 3):
            swap(kind, plane, step_f)

    def turn_last(kind, plane):
        arrive(kind, plane, 2, split=True)
        swap(kind, plane, 2)

    def passing(step, steps_f):
        for step_f in steps_f:
            arrive(0, planes[step], step_f)
            onward(0, planes[step], step_f)
            swap(0, planes[step], step_f)

    def climb(step):
        plane = planes[step]
        arrive(1, plane, 0)
        onward(1, plane, 0)
        around(1, plane, 0, 1)
        around(1, plane, 0, 3)
        swap(1, plane, 0)

    both_ways(1, 0)
    around(0, z, 0, 1)
    around(0, z, 0, 3)
    both_ways(0, 0)
    around(1, z, 0, 1)
    around(1, z, 0, 3)

    load_down.wait()
    scored = jnp.dot(down_buf[...], head_ref[...], preferred_element_type=jnp.float32)
    high = scored.astype(jnp.bfloat16)
    scored_buf[:, :actions_count] = high
    scored_buf[:, actions_count:] = (scored - high.astype(jnp.float32)).astype(jnp.bfloat16)

    tiles = hidden_units // TILE
    cuts = [tiles * number // 4 for number in range(5)]

    def compute(step):
        begin(step)
        more(step, 1)
        more(step, 2)
        finish(step)

    def begin(step):
        plane = planes[step]
        for step_f in ORDER:
            if step > 0 or step_f > 0:
                swapped(0, plane, step_f)
                swapped(1, plane, step_f)
        tile_span(plane, 0, cuts[1])

    def more(step, number):
        tile_span(planes[step], cuts[number], cuts[number + 1])

    def tile_span(plane, first, last):
        lhs_rows = RING * rows

        def tile(index, carry):
            at = pl.ds(pl.multiple_of(index * TILE, TILE), TILE)
            weights = jnp.concatenate([gate_buf[at, :], up_buf[at, :]], axis=0)
            lhs = jnp.concatenate(
                [
                    buffer[which, plane].reshape(lhs_rows, buffer.shape[-1])
                    for which in range(2)
                    for buffer in buffers
                ],
                axis=1,
            )
            both = lax.dot_general(
                lhs, weights, (((1,), (1,)), ((), ())), preferred_element_type=jnp.float32
            )
            hidden_buf[:, at] = (jax.nn.silu(both[:, :TILE]) * both[:, TILE:]).astype(
                jnp.bfloat16
            )
            return carry

        lax.fori_loop(first, last, tile, 0)

    def finish(step):
        tile_span(planes[step], cuts[3], tiles)
        result = jnp.dot(
            hidden_buf[...], scored_buf[...], preferred_element_type=jnp.float32
        )
        result = result[:, :actions_count] + result[:, actions_count:]
        result = result.reshape(RING, 2, half_rows, actions_count)
        partial[step, 0] = result[:, 0]
        partial[step, 1] = result[:, 1]
        send(
            partial.at[step, other],
            given.at[step],
            give_send.at[step],
            give_recv.at[step],
            device(0, 0, other),
        )

    def give_back(step):
        plane = planes[step]
        await_in(given.at[step], give_recv.at[step])
        sent[step] = (partial[step, core] + given[step]).astype(jnp.bfloat16)
        for step_f in range(RING):
            place = (p + step_f) % RING
            if (step, step_f) == (0, 0):
                landed[z, p] = sent[0, p]
            else:
                send(
                    sent.at[step, place],
                    landed.at[z, p],
                    back_send.at[RING * step + step_f],
                    back_recv.at[z * RING + (-step_f) % RING],
                    (gray(place), plane, core),
                )

    turn(0, z)
    both_ways(0, 1)
    both_ways(0, 3)
    climb(1)
    arrive(0, z, 2, split=True)
    both_ways(0, 2)
    swap(0, z, 2)
    turn(1, z)
    passing(1, (0, 1, 3))
    climb(2)
    turn_last(1, z)
    load_gate.wait()
    load_up.wait()
    begin(0)
    passing(1, (2,))
    more(0, 1)
    turn(1, planes[1])
    more(0, 2)
    passing(2, (0,))
    climb(3)
    finish(0)
    passing(2, (1,))
    turn_last(1, planes[1])
    begin(1)
    passing(2, (3,))
    more(1, 1)
    passing(2, (2,))
    turn(1, planes[2])
    more(1, 2)
    give_back(0)
    passing(3, (0,))
    finish(1)
    passing(3, (1,))
    turn_last(1, planes[2])
    begin(2)
    passing(3, (3,))
    more(2, 1)
    turn(1, planes[3])
    passing(3, (2,))
    more(2, 2)
    give_back(1)
    finish(2)
    turn_last(1, planes[3])
    compute(3)
    give_back(2)
    give_back(3)

    for step in range(RING):
        for step_f in range(RING):
            if (step, step_f) != (0, 0):
                await_in(
                    landed.at[planes[step], (p + step_f) % RING],
                    back_recv.at[planes[step] * RING + step_f],
                )
    mine = pl.ds(pl.multiple_of(core * half_rows, half_rows), half_rows)
    blended = jnp.zeros((half_rows, actions_count), jnp.float32)
    for expert in range(RING):
        part_sum = jnp.zeros((half_rows, actions_count), jnp.float32)
        for place in range(RING):
            part_sum = part_sum + landed[expert, place].astype(jnp.float32)
        blended = blended + share_buf[expert, mine, :] * part_sum
    halves[core] = blended
    send(
        halves.at[core], halves.at[core], pair_send.at[1], pair_recv.at[1], device(0, 0, other)
    )

    trace_row = trace_ref[...].astype(jnp.float32) / 1024.0
    trace_col = column(trace_row)
    reward_col = column(rewards_ref[...].astype(jnp.float32) * 0.25)
    action_col = column(actions_ref[...].astype(jnp.float32))
    log_row = jnp.log(DISCOUNT * trace_row)
    log_col = column(log_row)
    sums_row = jnp.sum(jnp.where(first_axis <= second_axis, log_col, 0.0), axis=0, keepdims=True)
    sums_col = jnp.sum(jnp.where(second_axis <= first_axis, log_row, 0.0), axis=1, keepdims=True)
    weight = jnp.where(
        first_axis >= second_axis, jnp.exp(jnp.minimum(sums_col - sums_row, 0.0)), 0.0
    )
    action_axis = lax.broadcasted_iota(jnp.int32, (rows, actions_count), 1).astype(jnp.float32)
    chosen = action_axis == action_col

    await_in(halves.at[other], pair_recv.at[1])
    values = jnp.concatenate([halves[0], halves[1]], axis=0)
    values_ref[...] = values
    greedy = jnp.max(values, axis=1, keepdims=True)
    taken = jnp.sum(jnp.where(chosen, values, 0.0), axis=1, keepdims=True)
    ahead_row = row_of(greedy - trace_col * taken)
    ahead = jnp.sum(
        jnp.where(second_axis == first_axis + 1, ahead_row, 0.0), axis=1, keepdims=True
    )
    driver = reward_col + DISCOUNT * ahead
    targets_ref[...] = jnp.sum(weight * driver, axis=0, keepdims=True)
    for condition, make in sends:
        if condition is None:
            make().wait_send()
        else:
            pl.when(condition)(lambda make=make: make().wait_send())


def per_device(
    tokens,
    norm_gain,
    expert_ids,
    gate_codes,
    gate_weights,
    up_weights,
    down_weights,
    value_head,
    actions,
    rewards,
    trace_codes,
):
    rows, wide = tokens.shape
    hidden_units, features = gate_weights.shape[1:]
    actions_count = value_head.shape[1]
    part = wide // 4
    held = (2, RING, RING, rows)
    half_rows = rows // 2
    vmem = pl.BlockSpec(memory_space=pltpu.VMEM)
    hbm = pl.BlockSpec(memory_space=pltpu.HBM)
    dma = pltpu.SemaphoreType.DMA
    blocks = RING * RING
    values, targets = pl.pallas_call(
        critic_kernel,
        out_shape=(
            jax.ShapeDtypeStruct((rows, actions_count), jnp.float32),
            jax.ShapeDtypeStruct((1, rows), jnp.float32),
        ),
        in_specs=[hbm, vmem, vmem, vmem, hbm, hbm, hbm, vmem, vmem, vmem, vmem],
        out_specs=(vmem, vmem),
        scratch_shapes=[
            pltpu.VMEM((2, rows, wide), jnp.bfloat16),
            pltpu.VMEM((*held, part), jnp.bfloat16),
            pltpu.VMEM((*held, wide - part), jnp.bfloat16),
            pltpu.VMEM((hidden_units, features), jnp.bfloat16),
            pltpu.VMEM((hidden_units, features), jnp.bfloat16),
            pltpu.VMEM((hidden_units, features), jnp.bfloat16),
            pltpu.VMEM((hidden_units, 2 * actions_count), jnp.bfloat16),
            pltpu.VMEM((RING * rows, hidden_units), jnp.bfloat16),
            pltpu.VMEM((RING, 2, RING, half_rows, actions_count), jnp.float32),
            pltpu.VMEM((RING, RING, half_rows, actions_count), jnp.float32),
            pltpu.VMEM((RING, RING, half_rows, actions_count), jnp.bfloat16),
            pltpu.VMEM((RING, RING, half_rows, actions_count), jnp.bfloat16),
            pltpu.VMEM((RING, rows, actions_count), jnp.float32),
            pltpu.VMEM((2, rows // 2, actions_count), jnp.float32),
            dma((4,)),
            dma((2,)),
            dma((2,)),
            dma((2, 5 * RING)),
            dma((2, 5 * RING)),
            dma((2, 2, blocks)),
            dma((2, blocks)),
            dma((2, blocks)),
            dma((RING,)),
            dma((RING,)),
            dma((blocks,)),
            dma((blocks,)),
        ],
        compiler_params=pltpu.CompilerParams(
            collective_id=0, has_side_effects=True, vmem_limit_bytes=60 * 1024 * 1024
        ),
    )(
        tokens,
        norm_gain.reshape(1, -1),
        expert_ids.T,
        gate_codes.T,
        gate_weights,
        up_weights,
        down_weights,
        value_head,
        actions.reshape(1, -1),
        rewards.reshape(1, -1),
        trace_codes.reshape(1, -1),
    )
    return values, targets.reshape(-1)


def solution(mesh):
    in_specs = (
        P(("dp", "expert"), "tensor"),
        P(),
        P(("dp", "expert"), None),
        P(("dp", "expert"), None),
        P("expert", ("dp", "tensor"), None),
        P("expert", ("dp", "tensor"), None),
        P("expert", ("dp", "tensor"), None),
        P(),
        P(("dp", "expert")),
        P(("dp", "expert")),
        P(("dp", "expert")),
    )
    out_specs = (P(("dp", "expert"), None), P(("dp", "expert")))
    shape = mesh.shape
    rings = shape["dp"] == RING and shape["expert"] == RING and shape["tensor"] == 2
    body = per_device if rings else per_device_plain
    return jax.shard_map(
        body, mesh=mesh, in_specs=in_specs, out_specs=out_specs, check_vma=False
    )
```
